32 devices in a mesh: sec: 4 (over y, core), op: 8 (over z, x).
Axes of the slice: x: 2, y: 2, z: 4, core: 2. Of those that a mesh axis runs over, the one named last changes fastest.
Arguments:
- wavefunction: bfloat16 [4, 512, 1024], P('sec', 'op'), may hold values from -4.5 to 4.5
- op_blocks: bfloat16 [8, 4, 1024, 1024], P('op', 'sec'), may hold values from -6 to 6
- basis_guess: bfloat16 [4, 1024, 512], P('sec'), may hold values from -4.5 to 4.5
- sector_sizes: int32 [4], replicated, may hold values from 768 to 1024
- kept_counts: int32 [4], replicated, may hold values from 256 to 512
- target_map: int32 [8, 4], replicated, may hold values from 0 to 3, as said below
- noise_numerator: int32 [1], replicated, may hold values from 256 to 1024
- noise_denominator: int32 [1], replicated, may hold values from 4194304 to 8388608
Outputs:
- kept_basis: float32 [4, 1024, 512], P('sec', 'op')
- rotated: float32 [8, 4, 512, 512], P('op', 'sec')
The draws below stay inside these ranges and needn't reach their ends.
Inputs may be any that keep to these rules, and one draw needn't show every extreme that they name: For every operator k, target_map[k] is a permutation of the 4 sectors.
All inputs are finite; a program needn't handle non-finite values.
Results may differ from the reference program's by a relative error of at most 0.005.
Values may be sent and summed in bfloat16 or wider, within the bound.
A program may use at most 64 MiB of HBM per device.

```python
import jax
import jax.numpy as jnp
from jax import lax

DIM = 1024
KEEP = 512
COLS = 512
SECTORS = 4
OPS = 8


def draw_target_map(key, part):
    operator_keys = jax.random.split(jax.random.fold_in(key, 17), OPS)
    orders = jax.vmap(lambda operator_key: jax.random.permutation(operator_key, SECTORS))(operator_keys)
    return orders.astype(jnp.int32)


def rough_rows(key, shape):
    values = jax.random.normal(jax.random.fold_in(key, 3), shape, jnp.float32)
    return jnp.clip(values, -4.5, 4.5)


def draw_wavefunction(key, part):
    return rough_rows(jax.random.fold_in(key, 29), (SECTORS, COLS, DIM)).astype(jnp.bfloat16)


def draw_basis_guess(key, part):
    return rough_rows(jax.random.fold_in(key, 31), (SECTORS, DIM, KEEP)).astype(jnp.bfloat16)


def set_ends(result, stream_key, least, high):
    spot = [jax.random.randint(jax.random.fold_in(stream_key, axis), (), 0, length) for axis, length in enumerate(result.shape)]
    widest = result.shape.index(max(result.shape))
    beside = spot[:widest] + [(spot[widest] + 1) % result.shape[widest]] + spot[widest + 1:]
    return result.at[tuple(spot)].set(least).at[tuple(beside)].set(high)


def block_levels(own_key, extent, pieces, smallest, top_value):
    loudness = 1.0
    for dim, parts in pieces:
        steps = jax.random.uniform(jax.random.fold_in(jax.random.fold_in(own_key, 6), dim), (parts,), jnp.float32, smallest / len(pieces), top_value / len(pieces))
        loudness = loudness * jnp.repeat(jnp.exp(steps), extent[dim] // parts).reshape((-1,) + (1,) * (len(extent) - 1 - dim))
    return loudness


def normal_values(own_key, dims, spread, bound, pieces=(), kind=jnp.bfloat16):
    values = spread * jax.random.normal(own_key, dims, jnp.float32)
    if pieces:
        values = values * block_levels(own_key, dims, pieces, -0.22, 0.18)
    return jnp.clip(values, -bound, bound).astype(kind)


def setup_inputs(seed: int = 0) -> dict:
    splits = jax.random.split(jax.random.key(seed), 9)
    return {
        "wavefunction": draw_wavefunction(jax.random.fold_in(splits[8], 71), 0),
        "op_blocks": normal_values(splits[1], (OPS, SECTORS, DIM, DIM), 1.0, 6.0, ((0, 8), (1, 4))),
        "basis_guess": draw_basis_guess(jax.random.fold_in(splits[8], 71), 0),
        "sector_sizes": set_ends(jax.random.randint(splits[3], (SECTORS,), 3 * DIM // 4, DIM + 1), jax.random.fold_in(splits[3], 1), 3 * DIM // 4, DIM).astype(jnp.int32),
        "kept_counts": set_ends(jax.random.randint(splits[4], (SECTORS,), KEEP // 2, KEEP + 1), jax.random.fold_in(splits[4], 1), KEEP // 2, KEEP).astype(jnp.int32),
        "target_map": draw_target_map(jax.random.fold_in(splits[8], 71), 0),
        "noise_numerator": jax.random.randint(splits[6], (1,), 256, 1025).astype(jnp.int32),
        "noise_denominator": jax.random.randint(splits[7], (1,), 4096 * DIM, 8192 * DIM + 1).astype(jnp.int32),
    }


def source_sectors(target_map):
    sectors = jnp.arange(SECTORS, dtype=jnp.int32)
    matches = target_map[:, :, None] == sectors[None, None, :]
    return jnp.sum(jnp.where(matches, sectors[None, :, None], 0), axis=1).astype(jnp.int32)

def reference(wavefunction, op_blocks, basis_guess, sector_sizes, kept_counts, target_map, noise_numerator, noise_denominator):
    highest = lax.Precision.HIGHEST
    noise_weight = noise_numerator[0].astype(jnp.float32) / noise_denominator[0].astype(jnp.float32)
    sources = source_sectors(target_map)
    states = jnp.arange(DIM, dtype=jnp.int32)
    state_mask = states[None, :] < sector_sizes[:, None]
    kept_mask = jnp.arange(KEEP, dtype=jnp.int32)[None, :] < kept_counts[:, None]
    masked = jnp.where(state_mask[:, None, :], wavefunction, jnp.zeros((), wavefunction.dtype))
    masked_wide = masked.astype(jnp.float32)
    base = jnp.einsum('scx,scy->sxy', masked_wide, masked_wide, precision=highest)

    def add_operator(running, inputs):
        blocks, anchor = inputs
        moved = jnp.take(masked_wide, anchor, axis=0)
        perturbed = jnp.einsum('tcx,txy->tcy', moved, blocks.astype(jnp.float32), precision=highest)
        perturbed = lax.optimization_barrier(perturbed.astype(jnp.bfloat16)).astype(jnp.float32)
        return (running + jnp.einsum('tcx,tcy->txy', perturbed, perturbed, precision=highest), None)
    noise_sum, unused = lax.scan(add_operator, jnp.zeros_like(base), (op_blocks, sources))
    density = base + noise_weight * noise_sum
    guess_masked = jnp.where(state_mask[:, :, None], basis_guess, jnp.zeros((), basis_guess.dtype)).astype(jnp.float32)
    image = jnp.einsum('sxy,syk->sxk', density, guess_masked, precision=highest)
    image = jnp.where(state_mask[:, :, None] & kept_mask[:, None, :], image, jnp.float32(0.0))
    padding = jnp.where(kept_mask, jnp.float32(0.0), jnp.float32(1.0))
    correlation = jnp.einsum('sdk,sdm->skm', image, image, precision=highest) + padding[:, :, None] * jnp.eye(KEEP, dtype=jnp.float32)[None]
    factor = jnp.linalg.cholesky(correlation)
    new_basis = lax.linalg.triangular_solve(factor, image, left_side=False, lower=True, transpose_a=True)
    kept_basis = new_basis * DIM ** 0.5
    basis_wide = lax.optimization_barrier(new_basis.astype(jnp.bfloat16)).astype(jnp.float32)

    def rotate(inputs):
        blocks, anchor = inputs
        mapped = jnp.einsum('txy,tyk->txk', blocks.astype(jnp.float32), basis_wide, precision=highest)
        mapped = lax.optimization_barrier(mapped.astype(jnp.bfloat16)).astype(jnp.float32)
        return jnp.einsum('txk,txm->tkm', jnp.take(basis_wide, anchor, axis=0), mapped, precision=highest)
    rotated = lax.map(rotate, (op_blocks, sources))
    return (kept_basis, rotated)
```

```python
import functools

import jax
import jax.numpy as jnp
from jax import lax
from jax.experimental import pallas as pl
from jax.experimental.pallas import tpu as pltpu
from jax.sharding import PartitionSpec as P

LANES = 128
ROWS = 8
HIGHEST = lax.Precision.HIGHEST


def dot_ta(a, b):
    return lax.dot_general(
        a, b, (((0,), (0,)), ((), ())), precision=HIGHEST, preferred_element_type=jnp.float32
    )


def dot(a, b):
    return jnp.dot(a, b, precision=HIGHEST, preferred_element_type=jnp.float32)


def eliminate_tile(tile):
    count = LANES // ROWS
    row = lax.broadcasted_iota(jnp.int32, (ROWS, LANES), 0)
    lane = lax.broadcasted_iota(jnp.int32, (ROWS, LANES), 1)
    left = [tile[ROWS * q : ROWS * (q + 1), :] for q in range(count)]
    right = [jnp.where(lane == row + ROWS * q, 1.0, 0.0).astype(jnp.float32) for q in range(count)]
    for p in range(count):
        upper, lower = left[p], right[p]
        columns = [
            jnp.broadcast_to(upper[:, ROWS * p + j : ROWS * p + j + 1], (ROWS, LANES))
            for j in range(ROWS)
        ]
        for j in range(ROWS):
            scale = lax.rsqrt(jnp.broadcast_to(columns[j][j : j + 1, :], (ROWS, LANES)))
            factor = jnp.where(row > j, columns[j] * scale, 0.0)
            for k in range(j + 1, ROWS):
                own = jnp.broadcast_to(columns[k][j : j + 1, :], (ROWS, LANES)) * scale
                columns[k] = columns[k] - factor * own
            own_upper = jnp.broadcast_to(upper[j : j + 1, :], (ROWS, LANES)) * scale
            own_lower = jnp.broadcast_to(lower[j : j + 1, :], (ROWS, LANES)) * scale
            upper = jnp.where(row == j, own_upper, upper - factor * own_upper)
            lower = jnp.where(row == j, own_lower, lower - factor * own_lower)
        right[p] = lower
        if p + 1 < count:
            change = dot_ta(upper, jnp.concatenate([upper, lower], axis=1))
            for q in range(p + 1, count):
                part = change[ROWS * q : ROWS * (q + 1), :]
                left[q] = left[q] - part[:, :LANES]
                right[q] = right[q] - part[:, LANES:]
    return jnp.concatenate(right, axis=0)


def inverse_factor_kernel(matrix_ref, out_ref, work):
    size = matrix_ref.shape[0]
    blocks = size // LANES
    work[:, :size] = matrix_ref[...]
    work[:, size:] = (
        lax.broadcasted_iota(jnp.int32, (size, size), 0)
        == lax.broadcasted_iota(jnp.int32, (size, size), 1)
    ).astype(jnp.float32)

    def step(b, carry):
        rows = pl.ds(pl.multiple_of(b * LANES, LANES), LANES)
        inverse = eliminate_tile(work[rows, rows])
        panel = dot(inverse, work[rows, :])
        work[rows, :] = panel
        out_ref[rows, :] = panel[:, size:]

        def update(i, inner):
            below = pl.ds(pl.multiple_of(i * LANES, LANES), LANES)
            work[below, :] = work[below, :] - dot_ta(work[rows, below], work[rows, :])
            return inner

        lax.fori_loop(b + 1, blocks, update, 0)
        return carry

    lax.fori_loop(0, blocks, step, 0)


def inverse_factor(matrix):
    size = matrix.shape[0]
    return pl.pallas_call(
        inverse_factor_kernel,
        out_shape=jax.ShapeDtypeStruct((size, size), jnp.float32),
        in_specs=[pl.BlockSpec(memory_space=pltpu.VMEM)],
        out_specs=pl.BlockSpec(memory_space=pltpu.VMEM),
        scratch_shapes=[pltpu.VMEM((size, 2 * size), jnp.float32)],
        compiler_params=pltpu.CompilerParams(vmem_limit_bytes=24 * 1024 * 1024),
        cost_estimate=pl.CostEstimate(flops=2 * size**3, bytes_accessed=8 * size * size, transcendentals=size),
        name="inverse_factor",
    )(matrix)


def source_sectors(target_map):
    sectors = jnp.arange(target_map.shape[1], dtype=jnp.int32)
    matches = target_map[:, :, None] == sectors[None, None, :]
    return jnp.sum(jnp.where(matches, sectors[None, :, None], 0), axis=1)


def fetch_pieces(own_slice, wanted_all):
    everyone = lax.all_gather(own_slice, "sec", axis=0, tiled=True)
    outgoing = jnp.take(everyone, wanted_all, axis=0)
    incoming = lax.all_to_all(outgoing, "op", split_axis=1, concat_axis=1, tiled=True)
    return incoming.reshape(
        incoming.shape[0], incoming.shape[1] * incoming.shape[2], incoming.shape[3]
    )


def body(
    wavefunction,
    op_blocks,
    basis_guess,
    sector_sizes,
    kept_counts,
    target_map,
    noise_numerator,
    noise_denominator,
):
    state_count = wavefunction.shape[2]
    kept_width = basis_guess.shape[2]
    tile_rows = state_count // lax.axis_size("op")
    sec_index = lax.axis_index("sec")
    op_index = lax.axis_index("op")
    noise_weight = noise_numerator[0].astype(jnp.float32) / noise_denominator[0].astype(jnp.float32)
    sources = source_sectors(target_map)
    wanted_all = lax.dynamic_index_in_dim(sources, sec_index, 1, keepdims=False)[None, :]
    wanted = lax.dynamic_index_in_dim(wanted_all[0], op_index, 0, keepdims=False)
    states = jnp.arange(state_count, dtype=jnp.int32)
    own_size = lax.dynamic_index_in_dim(sector_sizes, sec_index, 0, keepdims=False)
    source_size = lax.dynamic_index_in_dim(sector_sizes, wanted, 0, keepdims=False)
    own_count = lax.dynamic_index_in_dim(kept_counts, sec_index, 0, keepdims=False)
    own_kept = jnp.arange(kept_width, dtype=jnp.int32) < own_count
    zero_half = jnp.zeros((), jnp.bfloat16)
    own_rows = jnp.where((states < own_size)[None, :], wavefunction[0], zero_half)
    moved = fetch_pieces(wavefunction, wanted_all)[0]
    moved = jnp.where((states < source_size)[None, :], moved, zero_half)
    blocks = op_blocks[0, 0]
    perturbed = jnp.dot(moved, blocks, preferred_element_type=jnp.float32).astype(jnp.bfloat16)
    guess = jnp.where((states < own_size)[:, None], basis_guess[0], zero_half)
    perturbed_guess = noise_weight * jnp.dot(perturbed, guess, preferred_element_type=jnp.float32)
    own_guess = jnp.dot(own_rows, guess, preferred_element_type=jnp.float32)
    part = lax.dot_general(
        jnp.concatenate([perturbed, own_rows], axis=0).astype(jnp.float32),
        jnp.concatenate([perturbed_guess, own_guess], axis=0),
        (((0,), (0,)), ((), ())),
        precision=HIGHEST,
    )
    part = jnp.where((states < own_size)[:, None] & own_kept[None, :], part, jnp.float32(0.0))
    tile = lax.psum_scatter(part, "op", scatter_dimension=0, tiled=True)
    full_image = lax.all_gather(tile, "op", axis=0, tiled=True)
    padding = jnp.where(own_kept, jnp.float32(0.0), jnp.float32(1.0))
    correlation = dot_ta(full_image, full_image) + padding[:, None] * jnp.eye(
        kept_width, dtype=jnp.float32
    )
    inverse = inverse_factor(correlation)
    new_basis = lax.dot_general(
        full_image, inverse, (((1,), (1,)), ((), ())), precision=HIGHEST
    )
    kept_tile = (
        lax.dynamic_slice_in_dim(new_basis, op_index * tile_rows, tile_rows, 0)
        * float(state_count) ** 0.5
    )
    basis_half = new_basis.astype(jnp.bfloat16)
    mapped = jnp.dot(blocks, basis_half, preferred_element_type=jnp.float32).astype(jnp.bfloat16)
    own_tile = lax.dynamic_slice_in_dim(basis_half, op_index * tile_rows, tile_rows, 0)
    source_basis = fetch_pieces(own_tile[None], wanted_all)[0]
    rotated = lax.dot_general(
        source_basis, mapped, (((0,), (0,)), ((), ())), preferred_element_type=jnp.float32
    )
    return (kept_tile[None], rotated[None, None])


def solution(mesh):
    placed = (
        P("sec", "op", None),
        P("op", "sec", None, None),
        P("sec", None, None),
        P(),
        P(),
        P(),
        P(),
        P(),
    )
    return jax.shard_map(
        body,
        mesh=mesh,
        in_specs=placed,
        out_specs=(P("sec", "op", None), P("op", "sec", None, None)),
        check_vma=False,
    )
```

```python
import jax
import jax.numpy as jnp
from jax import lax
from jax.experimental import pallas as pl
from jax.experimental.pallas import tpu as pltpu
from jax.sharding import PartitionSpec as P

LANES = 128
ROWS = 8
HIGHEST = lax.Precision.HIGHEST


def dot_ta(a, b):
    return lax.dot_general(
        a, b, (((0,), (0,)), ((), ())), precision=HIGHEST, preferred_element_type=jnp.float32
    )


def dot(a, b):
    return jnp.dot(a, b, precision=HIGHEST, preferred_element_type=jnp.float32)


def eliminate_tile(tile):
    count = LANES // ROWS
    row = lax.broadcasted_iota(jnp.int32, (ROWS, LANES), 0)
    lane = lax.broadcasted_iota(jnp.int32, (ROWS, LANES), 1)
    left = [tile[ROWS * q : ROWS * (q + 1), :] for q in range(count)]
    right = [jnp.where(lane == row + ROWS * q, 1.0, 0.0).astype(jnp.float32) for q in range(count)]
    for p in range(count):
        upper, lower = left[p], right[p]
        columns = [
            jnp.broadcast_to(upper[:, ROWS * p + j : ROWS * p + j + 1], (ROWS, LANES))
            for j in range(ROWS)
        ]
        for j in range(ROWS):
            scale = lax.rsqrt(jnp.broadcast_to(columns[j][j : j + 1, :], (ROWS, LANES)))
            factor = jnp.where(row > j, columns[j] * scale, 0.0)
            for k in range(j + 1, ROWS):
                own = jnp.broadcast_to(columns[k][j : j + 1, :], (ROWS, LANES)) * scale
                columns[k] = columns[k] - factor * own
            own_upper = jnp.broadcast_to(upper[j : j + 1, :], (ROWS, LANES)) * scale
            own_lower = jnp.broadcast_to(lower[j : j + 1, :], (ROWS, LANES)) * scale
            upper = jnp.where(row == j, own_upper, upper - factor * own_upper)
            lower = jnp.where(row == j, own_lower, lower - factor * own_lower)
        right[p] = lower
        if p + 1 < count:
            change = dot_ta(upper, jnp.concatenate([upper, lower], axis=1))
            for q in range(p + 1, count):
                part = change[ROWS * q : ROWS * (q + 1), :]
                left[q] = left[q] - part[:, :LANES]
                right[q] = right[q] - part[:, LANES:]
    return jnp.concatenate(right, axis=0)


def inverse_factor_kernel(matrix_ref, out_ref, work):
    size = matrix_ref.shape[0]
    blocks = size // LANES
    work[:, :size] = matrix_ref[...]
    work[:, size:] = (
        lax.broadcasted_iota(jnp.int32, (size, size), 0)
        == lax.broadcasted_iota(jnp.int32, (size, size), 1)
    ).astype(jnp.float32)

    def step(b, carry):
        rows = pl.ds(pl.multiple_of(b * LANES, LANES), LANES)
        inverse = eliminate_tile(work[rows, rows])
        panel = dot(inverse, work[rows, :])
        work[rows, :] = panel
        out_ref[rows, :] = panel[:, size:]

        def update(i, inner):
            below = pl.ds(pl.multiple_of(i * LANES, LANES), LANES)
            work[below, :] = work[below, :] - dot_ta(work[rows, below], work[rows, :])
            return inner

        lax.fori_loop(b + 1, blocks, update, 0)
        return carry

    lax.fori_loop(0, blocks, step, 0)


def inverse_factor(matrix):
    size = matrix.shape[0]
    return pl.pallas_call(
        inverse_factor_kernel,
        out_shape=jax.ShapeDtypeStruct((size, size), jnp.float32),
        in_specs=[pl.BlockSpec(memory_space=pltpu.VMEM)],
        out_specs=pl.BlockSpec(memory_space=pltpu.VMEM),
        scratch_shapes=[pltpu.VMEM((size, 2 * size), jnp.float32)],
        compiler_params=pltpu.CompilerParams(vmem_limit_bytes=24 * 1024 * 1024),
        cost_estimate=pl.CostEstimate(flops=2 * size**3, bytes_accessed=8 * size * size, transcendentals=size),
        name="inverse_factor",
    )(matrix)


def source_sectors(target_map):
    sectors = jnp.arange(target_map.shape[1], dtype=jnp.int32)
    matches = target_map[:, :, None] == sectors[None, None, :]
    return jnp.sum(jnp.where(matches, sectors[None, :, None], 0), axis=1)


def fetch_pieces(own_slice, wanted_all):
    everyone = lax.all_gather(own_slice, "sec", axis=0, tiled=True)
    outgoing = jnp.take(everyone, wanted_all, axis=0)
    incoming = lax.all_to_all(outgoing, "op", split_axis=1, concat_axis=1, tiled=True)
    return incoming.reshape(
        incoming.shape[0], incoming.shape[1] * incoming.shape[2], incoming.shape[3]
    )


def exchange(value, axis, bit):
    count = lax.axis_size(axis)
    return lax.ppermute(value, axis, [(i, i ^ bit) for i in range(count)])


def halves(value, side):
    half = value.shape[0] // 2
    kept = lax.dynamic_slice_in_dim(value, side * half, half, 0)
    given = lax.dynamic_slice_in_dim(value, (1 - side) * half, half, 0)
    return kept, given


def sum_over_op(value):
    count = lax.axis_size("op")
    index = lax.axis_index("op")
    bits = [1 << b for b in range(count.bit_length() - 1)]
    orders = [bits, bits[1:] + bits[:1]]
    half = value.shape[0] // 2
    held = [value[:half], value[half:]]
    for step in range(len(bits)):
        for color, order in enumerate(orders):
            kept, given = halves(held[color], (index // order[step]) % 2)
            held[color] = kept + exchange(given, "op", order[step])
    for step in reversed(range(len(bits))):
        for color, order in enumerate(orders):
            own = held[color]
            other = exchange(own, "op", order[step])
            first = (index // order[step]) % 2 == 0
            held[color] = jnp.concatenate(
                [jnp.where(first, own, other), jnp.where(first, other, own)], axis=0
            )
    return jnp.concatenate(held, axis=0)


def fetch_sector(own, wanted):
    count = lax.axis_size("sec")
    offset = lax.axis_index("sec") ^ wanted
    held = {0: own}
    bit = count // 2
    while bit:
        for known in list(held):
            held[known ^ bit] = exchange(held[known], "sec", bit)
        bit //= 2
    result = own
    for known, value in held.items():
        result = jnp.where(offset == known, value, result)
    return result


def body(
    wavefunction,
    op_blocks,
    basis_guess,
    sector_sizes,
    kept_counts,
    target_map,
    noise_numerator,
    noise_denominator,
):
    state_count = wavefunction.shape[2]
    kept_width = basis_guess.shape[2]
    tile_rows = state_count // lax.axis_size("op")
    sec_index = lax.axis_index("sec")
    op_index = lax.axis_index("op")
    noise_weight = noise_numerator[0].astype(jnp.float32) / noise_denominator[0].astype(jnp.float32)
    sources = source_sectors(target_map)
    wanted_all = lax.dynamic_index_in_dim(sources, sec_index, 1, keepdims=False)[None, :]
    wanted = lax.dynamic_index_in_dim(wanted_all[0], op_index, 0, keepdims=False)
    states = jnp.arange(state_count, dtype=jnp.int32)
    own_size = lax.dynamic_index_in_dim(sector_sizes, sec_index, 0, keepdims=False)
    source_size = lax.dynamic_index_in_dim(sector_sizes, wanted, 0, keepdims=False)
    own_count = lax.dynamic_index_in_dim(kept_counts, sec_index, 0, keepdims=False)
    own_kept = jnp.arange(kept_width, dtype=jnp.int32) < own_count
    zero_half = jnp.zeros((), jnp.bfloat16)
    own_rows = jnp.where((states < own_size)[None, :], wavefunction[0], zero_half)
    moved = fetch_pieces(wavefunction, wanted_all)[0]
    moved = jnp.where((states < source_size)[None, :], moved, zero_half)
    blocks = op_blocks[0, 0]
    perturbed = jnp.dot(moved, blocks, preferred_element_type=jnp.float32).astype(jnp.bfloat16)
    guess = jnp.where((states < own_size)[:, None], basis_guess[0], zero_half)
    perturbed_guess = noise_weight * jnp.dot(perturbed, guess, preferred_element_type=jnp.float32)
    own_guess = jnp.dot(own_rows, guess, preferred_element_type=jnp.float32)
    part = lax.dot_general(
        jnp.concatenate([perturbed, own_rows], axis=0).astype(jnp.float32),
        jnp.concatenate([perturbed_guess, own_guess], axis=0),
        (((0,), (0,)), ((), ())),
        precision=lax.Precision.HIGH,
    )
    part = jnp.where((states < own_size)[:, None] & own_kept[None, :], part, jnp.float32(0.0))
    full_image = sum_over_op(part)
    padding = jnp.where(own_kept, jnp.float32(0.0), jnp.float32(1.0))
    correlation = dot_ta(full_image, full_image) + padding[:, None] * jnp.eye(
        kept_width, dtype=jnp.float32
    )
    inverse = inverse_factor(correlation)
    new_basis = lax.dot_general(
        full_image, inverse, (((1,), (1,)), ((), ())), precision=lax.Precision.HIGH
    )
    kept_tile = (
        lax.dynamic_slice_in_dim(new_basis, op_index * tile_rows, tile_rows, 0)
        * float(state_count) ** 0.5
    )
    basis_half = new_basis.astype(jnp.bfloat16)
    mapped = jnp.dot(blocks, basis_half, preferred_element_type=jnp.float32).astype(jnp.bfloat16)
    source_basis = fetch_sector(basis_half, wanted)
    rotated = lax.dot_general(
        source_basis, mapped, (((0,), (0,)), ((), ())), preferred_element_type=jnp.float32
    )
    return (kept_tile[None], rotated[None, None])


def solution(mesh):
    placed = (
        P("sec", "op", None),
        P("op", "sec", None, None),
        P("sec", None, None),
        P(),
        P(),
        P(),
        P(),
        P(),
    )
    return jax.shard_map(
        body,
        mesh=mesh,
        in_specs=placed,
        out_specs=(P("sec", "op", None), P("op", "sec", None, None)),
        check_vma=False,
    )
```
